32 devices in a mesh: gx: 2 (over x), gy: 16 (over z, y, core).
Axes of the slice: x: 2, y: 2, z: 4, core: 2. Of those that a mesh axis runs over, the one named last changes fastest.
Arguments:
- weights: float32 [131072], P(('gx', 'gy')), may hold values from -6 to 6
- bin_ids: int32 [131072], P(('gx', 'gy')), may hold values from 0 to 4095
Outputs:
- significance: float32 [4096], P(('gx', 'gy'))
- overall: float32 [], replicated
The draws below stay inside these ranges and needn't reach their ends.
Inputs may be any that keep to these rules, and one draw needn't show every extreme that they name: `bin_ids`: every bin id lies in 0 to 4095.
All inputs are finite; a program needn't handle non-finite values.
Results may differ from the reference program's by a relative error of at most 0.0003.
Values sent between devices are 32-bit elements.
A program may use at most 64 MiB of HBM per device.

```python
import math
import jax
import jax.numpy as jnp
import numpy as np

EVENTS = 131072
BINS = 4096


def plant(values, key, low, high):
    index_at = [jax.random.randint(jax.random.fold_in(key, axis), (), 0, length) for axis, length in enumerate(values.shape)]
    widest = values.shape.index(max(values.shape))
    neighbour = index_at[:widest] + [(index_at[widest] + 1) % values.shape[widest]] + index_at[widest + 1:]
    return values.at[tuple(index_at)].set(low).at[tuple(neighbour)].set(high)


def steps_of(own_key, shape, shards, least, high):
    def one(dim, blocks):
        steps = jax.random.uniform(jax.random.fold_in(jax.random.fold_in(own_key, 6), dim), (blocks,), jnp.float32, least / len(shards), high / len(shards))
        return jnp.repeat(jnp.exp(steps), shape[dim] // blocks).reshape((-1,) + (1,) * (len(shape) - dim - 1))

    level = one(*shards[0])
    for cut in shards[1:]:
        level = level * one(*cut)
    return level


def cumulative_ranks(number_of, skew):
    portions = [(1 << 20) // math.isqrt(rank ** skew) + 1 for rank in range(1, number_of + 1)]
    deviation = 1 + sum(portions) // (1 << 30)
    return np.cumsum(np.array([max(1, weight // deviation) for weight in portions]))


def skewed_ids(key, dims, number_of, lean):
    table = cumulative_ranks(number_of, lean)
    pick = jax.random.randint(jax.random.fold_in(key, 1), dims, 0, int(table[number_of - 1]))
    standing = jnp.searchsorted(jnp.asarray(table, jnp.int32), pick, side="right")
    return jax.random.permutation(jax.random.fold_in(key, 2), number_of)[standing].astype(jnp.int32)


def gaussian(key, shape, spread, most, pieces=(), dtype=jnp.bfloat16):
    gain = steps_of(key, shape, pieces, -0.22, 0.18) if pieces else 1.0
    values = jax.random.normal(key, shape, jnp.float32) * spread * gain
    return jnp.minimum(jnp.maximum(values, -most), most).astype(dtype)


def setup_inputs(seed: int = 0) -> dict:
    splits = jax.random.split(jax.random.key(seed), 3)
    weights = gaussian(splits[0], (EVENTS,), 1.0, 6.0, ((0, 32),), jnp.float32)
    bin_ids = plant(skewed_ids(splits[1], (EVENTS,), BINS, 1), jax.random.fold_in(splits[1], 3), 0, BINS - 1).astype(jnp.int32)
    return {"weights": weights, "bin_ids": bin_ids}


def reference(weights, bin_ids):
    sumw = jax.ops.segment_sum(weights, bin_ids, num_segments=BINS)
    sumw2 = jax.ops.segment_sum(weights * weights, bin_ids, num_segments=BINS)
    significance = sumw / jnp.sqrt(sumw2 + 1.0)
    overall = jnp.sum(sumw) / jnp.sqrt(jnp.sum(sumw2) + 1.0)
    return (significance, overall)
```

```python
import functools

import jax
import jax.numpy as jnp
from jax import lax
from jax.experimental import pallas as pl
from jax.experimental.pallas import tpu as pltpu
from jax.sharding import PartitionSpec as P

LANES = 128


def split(x):
    high = x.astype(jnp.bfloat16)
    low = (x - high.astype(jnp.float32)).astype(jnp.bfloat16)
    return high, low


def local_histogram(n, w, ids):
    rows = w.shape[0]
    lane_iota = lax.broadcasted_iota(jnp.int32, (LANES, LANES), 0)
    dev_iota = lax.broadcasted_iota(jnp.int32, (n, LANES), 0)
    total = jnp.zeros((4 * n, LANES), jnp.float32)
    w_parts = split(w)
    q_parts = split(w * w)
    values = [v.astype(jnp.float32) for v in (*w_parts, *q_parts)]
    owner, lane = ids // LANES, ids % LANES
    left, right = [], []
    for r in range(rows):
        right.append(jnp.where(lane_iota == lane[r : r + 1], 1.0, 0.0).astype(jnp.bfloat16))
        mine = dev_iota == owner[r : r + 1]
        left.append(jnp.concatenate([jnp.where(mine, v[r : r + 1], 0.0) for v in values], axis=0).astype(jnp.bfloat16))
    total = lax.dot_general(
        jnp.concatenate(left, axis=1),
        jnp.concatenate(right, axis=1),
        (((1,), (1,)), ((), ())),
        preferred_element_type=jnp.float32,
    )
    return total[:n] + total[n : 2 * n], total[2 * n : 3 * n] + total[3 * n :]


def kernel(nx, ny, w_ref, ids_ref, out_ref, held, arrived, send_sem, recv_sem):
    n = nx * ny
    me = lax.axis_index("gx") * ny + lax.axis_index("gy")

    def partner(k):
        other = lax.rem(me + k, n)
        return other, (other // ny, lax.rem(other, ny))

    barrier = pltpu.get_barrier_semaphore()
    for k in range(1, n):
        pl.semaphore_signal(barrier, inc=1, device_id=partner(k)[1], device_id_type=pl.DeviceIdType.MESH)

    w = w_ref[...]
    sums, squares = local_histogram(n, w, ids_ref[...])
    part_sum = jnp.sum(w, axis=0, keepdims=True)
    part_sq = jnp.sum(w * w, axis=0, keepdims=True)
    for d in range(n):
        held[d] = jnp.concatenate([sums[d : d + 1], squares[d : d + 1], part_sum, part_sq], axis=0)

    pl.semaphore_wait(barrier, n - 1)
    for k in range(1, n):
        other, where = partner(k)
        pltpu.make_async_remote_copy(
            src_ref=held.at[other],
            dst_ref=arrived.at[k - 1],
            send_sem=send_sem,
            recv_sem=recv_sem,
            device_id=where,
            device_id_type=pl.DeviceIdType.MESH,
        ).start()
    own = held[me]
    pltpu.make_async_copy(arrived, arrived, recv_sem).wait()
    total = own + jnp.sum(arrived[...], axis=0)
    significance = total[0:1] / jnp.sqrt(total[1:2] + 1.0)
    whole = jnp.sum(total[2:4], axis=1, keepdims=True)
    overall = whole[0:1] / jnp.sqrt(whole[1:2] + 1.0)
    out_ref[0:1] = significance
    out_ref[1:2] = jnp.broadcast_to(overall, (1, LANES))
    pltpu.make_async_copy(arrived, arrived, send_sem).wait()


def shards(nx, ny, weights, bin_ids):
    n = nx * ny
    vmem = pl.BlockSpec(memory_space=pltpu.VMEM)
    out = pl.pallas_call(
        functools.partial(kernel, nx, ny),
        out_shape=jax.ShapeDtypeStruct((2, LANES), jnp.float32),
        in_specs=[vmem, vmem],
        out_specs=vmem,
        scratch_shapes=[
            pltpu.VMEM((n, 4, LANES), jnp.float32),
            pltpu.VMEM((n - 1, 4, LANES), jnp.float32),
            pltpu.SemaphoreType.DMA,
            pltpu.SemaphoreType.DMA,
        ],
        compiler_params=pltpu.CompilerParams(collective_id=0, has_side_effects=True),
    )(weights.reshape(-1, LANES), bin_ids.reshape(-1, LANES))
    return out[0], out[1, 0]


def solution(mesh):
    spec = P(("gx", "gy"))
    body = functools.partial(shards, mesh.shape["gx"], mesh.shape["gy"])
    return jax.shard_map(body, mesh=mesh, in_specs=(spec, spec), out_specs=(spec, P()), check_vma=False)
```

```python
import functools

import jax
import jax.numpy as jnp
from jax import lax
from jax.experimental import pallas as pl
from jax.experimental.pallas import tpu as pltpu
from jax.sharding import PartitionSpec as P

LANES = 128
ROWS = 3
ORDER = 0
WHAT = 0


def split(x):
    high = x.astype(jnp.bfloat16).astype(jnp.float32)
    return high, x - high


def local_histogram(n, w, ids):
    lane_iota = lax.broadcasted_iota(jnp.int32, (LANES, LANES), 0)
    dev_iota = lax.broadcasted_iota(jnp.int32, (n, LANES), 0)
    values = (*split(w), *split(w * w))
    owner, lane = ids // LANES, ids % LANES
    left, right = [], []
    for r in range(w.shape[0]):
        one = slice(r, r + 1)
        right.append(jnp.where(lane_iota == lane[one], 1.0, 0.0).astype(jnp.bfloat16))
        mine = dev_iota == owner[one]
        left.append(jnp.concatenate([jnp.where(mine, v[one], 0.0) for v in values], axis=0).astype(jnp.bfloat16))
    total = lax.dot_general(
        jnp.concatenate(left, axis=1),
        jnp.concatenate(right, axis=1),
        (((1,), (1,)), ((), ())),
        preferred_element_type=jnp.float32,
    )
    return total[:n] + total[n : 2 * n], total[2 * n : 3 * n] + total[3 * n :]


def partials(w):
    rows = [jnp.sum(w, axis=0, keepdims=True), jnp.sum(w * w, axis=0, keepdims=True)]
    if ROWS == 4:
        return rows
    half = LANES // 2
    folded = [r + pltpu.roll(r, half, 1) for r in rows]
    return [jnp.where(lax.broadcasted_iota(jnp.int32, (1, LANES), 1) < half, *folded)]


def kernel(nx, ny, w_hbm, ids_hbm, out_ref, w_ref, ids_ref, held, arrived, send_sem, recv_sem, load_sems):
    n = nx * ny
    loads = [
        pltpu.make_async_copy(w_hbm, w_ref, load_sems.at[0]),
        pltpu.make_async_copy(ids_hbm, ids_ref, load_sems.at[1]),
    ]
    for load in loads:
        load.start()
    me = lax.axis_index("gx") * ny + lax.axis_index("gy")

    def place(other):
        return (other // ny, other % ny)

    if ORDER == 0:
        ks = list(range(1, n))
    else:
        ks = [k for j in range(n // 2) for k in (n // 2 - j, n // 2 + j) if 0 < k < n]
        ks = sorted(set(ks), key=ks.index)

    barrier = pltpu.get_barrier_semaphore()
    for k in ks:
        pl.semaphore_signal(barrier, inc=1, device_id=place((me + k) % n), device_id_type=pl.DeviceIdType.MESH)

    for load in loads:
        load.wait()
    w = w_ref[...]
    if WHAT != 2:
        sums, squares = local_histogram(n, w, ids_ref[...])
    else:
        sums = jnp.broadcast_to(w[0:1], (n, LANES))
        squares = sums
    parts = partials(w)
    for d in range(n):
        held[d] = jnp.concatenate([sums[d : d + 1], squares[d : d + 1], *parts], axis=0)

    pl.semaphore_wait(barrier, n - 1)
    for k in ks:
        other = (me + k) % n
        pltpu.make_async_remote_copy(
            src_ref=held.at[other],
            dst_ref=arrived.at[k - 1],
            send_sem=send_sem,
            recv_sem=recv_sem,
            device_id=place(other),
            device_id_type=pl.DeviceIdType.MESH,
        ).start()
    own = held[me]
    pltpu.make_async_copy(arrived, arrived, recv_sem).wait()
    out_ref[...] = own + jnp.sum(arrived[...], axis=0)
    pltpu.make_async_copy(arrived, arrived, send_sem).wait()


def finish_kernel(total_ref, sig_ref, all_ref):
    total = total_ref[...]
    sig_ref[...] = total[0:1] / jnp.sqrt(total[1:2] + 1.0)
    if ROWS == 4:
        whole = jnp.sum(total[2:4], axis=1, keepdims=True)
        a, b = whole[0:1], whole[1:2]
    else:
        half = LANES // 2
        a = jnp.sum(total[2:3, :half], axis=1, keepdims=True)
        b = jnp.sum(total[2:3, half:], axis=1, keepdims=True)
    all_ref[...] = a / jnp.sqrt(b + 1.0)


def shards(nx, ny, weights, bin_ids):
    n = nx * ny
    vmem = pl.BlockSpec(memory_space=pltpu.VMEM)
    hbm = pl.BlockSpec(memory_space=pltpu.HBM)
    weights, bin_ids = weights.reshape(-1, LANES), bin_ids.reshape(-1, LANES)
    total = pl.pallas_call(
        functools.partial(kernel, nx, ny),
        out_shape=jax.ShapeDtypeStruct((ROWS, LANES), jnp.float32),
        in_specs=[hbm, hbm],
        out_specs=vmem,
        scratch_shapes=[
            pltpu.VMEM(weights.shape, weights.dtype),
            pltpu.VMEM(bin_ids.shape, bin_ids.dtype),
            pltpu.VMEM((n, ROWS, LANES), jnp.float32),
            pltpu.VMEM((n - 1, ROWS, LANES), jnp.float32),
            pltpu.SemaphoreType.DMA,
            pltpu.SemaphoreType.DMA,
            pltpu.SemaphoreType.DMA((2,)),
        ],
        compiler_params=pltpu.CompilerParams(
            collective_id=0, has_side_effects=True, vmem_limit_bytes=16 * 1024 * 1024
        ),
    )(weights, bin_ids)
    significance, overall = pl.pallas_call(
        finish_kernel,
        out_shape=(jax.ShapeDtypeStruct((1, LANES), jnp.float32), jax.ShapeDtypeStruct((1, 1), jnp.float32)),
        in_specs=[vmem],
        out_specs=(vmem, vmem),
        compiler_params=pltpu.CompilerParams(vmem_limit_bytes=16 * 1024 * 1024),
    )(total)
    return significance.reshape(LANES), overall.reshape(())


def solution(mesh):
    spec = P(("gx", "gy"))
    body = functools.partial(shards, mesh.shape["gx"], mesh.shape["gy"])
    return jax.shard_map(body, mesh=mesh, in_specs=(spec, spec), out_specs=(spec, P()), check_vma=False)
```

```python
import functools

import jax
import jax.numpy as jnp
from jax import lax
from jax.experimental import pallas as pl
from jax.experimental.pallas import tpu as pltpu
from jax.sharding import PartitionSpec as P

LANES = 128
ROWS = 3
ORDER = 0
WHAT = 0


def split(x):
    high = x.astype(jnp.bfloat16).astype(jnp.float32)
    return high, x - high


def local_histogram(n, w, ids):
    lane_iota = lax.broadcasted_iota(jnp.int32, (LANES, LANES), 0)
    dev_iota = lax.broadcasted_iota(jnp.int32, (n, LANES), 0)
    values = (*split(w), *split(w * w))
    owner, lane = ids // LANES, ids % LANES
    left, right = [], []
    for r in range(w.shape[0]):
        one = slice(r, r + 1)
        right.append(jnp.where(lane_iota == lane[one], 1.0, 0.0).astype(jnp.bfloat16))
        mine = dev_iota == owner[one]
        left.append(jnp.concatenate([jnp.where(mine, v[one], 0.0) for v in values], axis=0).astype(jnp.bfloat16))
    total = lax.dot_general(
        jnp.concatenate(left, axis=1),
        jnp.concatenate(right, axis=1),
        (((1,), (1,)), ((), ())),
        preferred_element_type=jnp.float32,
    )
    return total[:n] + total[n : 2 * n], total[2 * n : 3 * n] + total[3 * n :]


def partials(w):
    rows = [jnp.sum(w, axis=0, keepdims=True), jnp.sum(w * w, axis=0, keepdims=True)]
    if ROWS == 4:
        return rows
    half = LANES // 2
    folded = [r + pltpu.roll(r, half, 1) for r in rows]
    return [jnp.where(lax.broadcasted_iota(jnp.int32, (1, LANES), 1) < half, *folded)]


def kernel(nx, ny, w_hbm, ids_hbm, out_ref, w_ref, ids_ref, held, arrived, send_sem, recv_sem, load_sems):
    n = nx * ny
    loads = [
        pltpu.make_async_copy(w_hbm, w_ref, load_sems.at[0]),
        pltpu.make_async_copy(ids_hbm, ids_ref, load_sems.at[1]),
    ]
    for load in loads:
        load.start()
    me = lax.axis_index("gx") * ny + lax.axis_index("gy")

    def place(other):
        return (other // ny, other % ny)

    if ORDER == 0:
        ks = list(range(1, n))
    else:
        ks = [k for j in range(n // 2) for k in (n // 2 - j, n // 2 + j) if 0 < k < n]
        ks = sorted(set(ks), key=ks.index)

    barrier = pltpu.get_barrier_semaphore()
    for k in ks:
        pl.semaphore_signal(barrier, inc=1, device_id=place((me + k) % n), device_id_type=pl.DeviceIdType.MESH)

    for load in loads:
        load.wait()
    w = w_ref[...]
    if WHAT != 2:
        sums, squares = local_histogram(n, w, ids_ref[...])
    else:
        sums = jnp.broadcast_to(w[0:1], (n, LANES))
        squares = sums
    parts = partials(w)
    for d in range(n):
        held[d] = jnp.concatenate([sums[d : d + 1], squares[d : d + 1], *parts], axis=0)

    pl.semaphore_wait(barrier, n - 1)
    for k in ks:
        other = (me + k) % n
        pltpu.make_async_remote_copy(
            src_ref=held.at[other],
            dst_ref=arrived.at[k - 1],
            send_sem=send_sem,
            recv_sem=recv_sem,
            device_id=place(other),
            device_id_type=pl.DeviceIdType.MESH,
        ).start()
    own = held[me]
    pltpu.make_async_copy(arrived, arrived, recv_sem).wait()
    out_ref[...] = own + jnp.sum(arrived[...], axis=0)
    pltpu.make_async_copy(arrived, arrived, send_sem).wait()


def finish_kernel(total_ref, sig_ref, all_ref):
    total = total_ref[...]
    sig_ref[...] = total[0:1] / jnp.sqrt(total[1:2] + 1.0)
    if ROWS == 4:
        whole = jnp.sum(total[2:4], axis=1, keepdims=True)
        a, b = whole[0:1], whole[1:2]
    else:
        half = LANES // 2
        a = jnp.sum(total[2:3, :half], axis=1, keepdims=True)
        b = jnp.sum(total[2:3, half:], axis=1, keepdims=True)
    all_ref[...] = a / jnp.sqrt(b + 1.0)


def shards(nx, ny, weights, bin_ids):
    n = nx * ny
    vmem = pl.BlockSpec(memory_space=pltpu.VMEM)
    hbm = pl.BlockSpec(memory_space=pltpu.HBM)
    weights, bin_ids = weights.reshape(-1, LANES), bin_ids.reshape(-1, LANES)
    total = pl.pallas_call(
        functools.partial(kernel, nx, ny),
        out_shape=pltpu.VMEM((ROWS, LANES), jnp.float32),
        in_specs=[hbm, hbm],
        out_specs=vmem,
        scratch_shapes=[
            pltpu.VMEM(weights.shape, weights.dtype),
            pltpu.VMEM(bin_ids.shape, bin_ids.dtype),
            pltpu.VMEM((n, ROWS, LANES), jnp.float32),
            pltpu.VMEM((n - 1, ROWS, LANES), jnp.float32),
            pltpu.SemaphoreType.DMA,
            pltpu.SemaphoreType.DMA,
            pltpu.SemaphoreType.DMA((2,)),
        ],
        compiler_params=pltpu.CompilerParams(
            collective_id=0, has_side_effects=True, vmem_limit_bytes=67043328 - 8192
        ),
    )(weights, bin_ids)
    significance, overall = pl.pallas_call(
        finish_kernel,
        out_shape=(jax.ShapeDtypeStruct((1, LANES), jnp.float32), jax.ShapeDtypeStruct((1, 1), jnp.float32)),
        in_specs=[vmem],
        out_specs=(vmem, vmem),
        compiler_params=pltpu.CompilerParams(vmem_limit_bytes=67043328 - 8192),
    )(total)
    return significance.reshape(LANES), overall.reshape(())


def solution(mesh):
    spec = P(("gx", "gy"))
    body = functools.partial(shards, mesh.shape["gx"], mesh.shape["gy"])
    return jax.shard_map(body, mesh=mesh, in_specs=(spec, spec), out_specs=(spec, P()), check_vma=False)
```

```python
import functools

import jax
import jax.numpy as jnp
from jax import lax
from jax.experimental import pallas as pl
from jax.experimental.pallas import tpu as pltpu
from jax.sharding import PartitionSpec as P

LANES = 128
ROWS = 3
ORDER = 0
WHAT = 0


def split(x):
    high = x.astype(jnp.bfloat16).astype(jnp.float32)
    return high, x - high


def local_histogram(n, w, ids):
    lane_iota = lax.broadcasted_iota(jnp.int32, (LANES, LANES), 0)
    dev_iota = lax.broadcasted_iota(jnp.int32, (n, LANES), 0)
    values = (*split(w), *split(w * w))
    owner, lane = ids // LANES, ids % LANES
    left, right = [], []
    for r in range(w.shape[0]):
        one = slice(r, r + 1)
        right.append(jnp.where(lane_iota == lane[one], 1.0, 0.0).astype(jnp.bfloat16))
        mine = dev_iota == owner[one]
        left.append(jnp.concatenate([jnp.where(mine, v[one], 0.0) for v in values], axis=0).astype(jnp.bfloat16))
    total = lax.dot_general(
        jnp.concatenate(left, axis=1),
        jnp.concatenate(right, axis=1),
        (((1,), (1,)), ((), ())),
        preferred_element_type=jnp.float32,
    )
    return total[:n] + total[n : 2 * n], total[2 * n : 3 * n] + total[3 * n :]


def partials(w):
    rows = [jnp.sum(w, axis=0, keepdims=True), jnp.sum(w * w, axis=0, keepdims=True)]
    if ROWS == 4:
        return rows
    half = LANES // 2
    folded = [r + pltpu.roll(r, half, 1) for r in rows]
    return [jnp.where(lax.broadcasted_iota(jnp.int32, (1, LANES), 1) < half, *folded)]


def kernel(nx, ny, w_hbm, ids_hbm, out_ref, w_ref, ids_ref, held, arrived, send_sem, recv_sem, load_sems):
    n = nx * ny
    loads = [
        pltpu.make_async_copy(w_hbm, w_ref, load_sems.at[0]),
        pltpu.make_async_copy(ids_hbm, ids_ref, load_sems.at[1]),
    ]
    for load in loads:
        load.start()
    me = lax.axis_index("gx") * ny + lax.axis_index("gy")

    def place(other):
        return (other // ny, other % ny)

    if ORDER == 0:
        ks = list(range(1, n))
    else:
        ks = [k for j in range(n // 2) for k in (n // 2 - j, n // 2 + j) if 0 < k < n]
        ks = sorted(set(ks), key=ks.index)

    barrier = pltpu.get_barrier_semaphore()
    for k in ks:
        pl.semaphore_signal(barrier, inc=1, device_id=place((me + k) % n), device_id_type=pl.DeviceIdType.MESH)

    for load in loads:
        load.wait()
    w = w_ref[...]
    if WHAT != 2:
        sums, squares = local_histogram(n, w, ids_ref[...])
    else:
        sums = jnp.broadcast_to(w[0:1], (n, LANES))
        squares = sums
    parts = partials(w)
    for d in range(n):
        held[d] = jnp.concatenate([sums[d : d + 1], squares[d : d + 1], *parts], axis=0)

    pl.semaphore_wait(barrier, n - 1)
    for k in ks:
        other = (me + k) % n
        pltpu.make_async_remote_copy(
            src_ref=held.at[other],
            dst_ref=arrived.at[k - 1],
            send_sem=send_sem,
            recv_sem=recv_sem,
            device_id=place(other),
            device_id_type=pl.DeviceIdType.MESH,
        ).start()
    own = held[me]
    pltpu.make_async_copy(arrived, arrived, recv_sem).wait()
    out_ref[...] = own + jnp.sum(arrived[...], axis=0)
    pltpu.make_async_copy(arrived, arrived, send_sem).wait()


def finish_kernel(total_ref, sig_ref, all_ref):
    total = total_ref[...]
    sig_ref[...] = total[0:1] / jnp.sqrt(total[1:2] + 1.0)
    if ROWS == 4:
        whole = jnp.sum(total[2:4], axis=1, keepdims=True)
        a, b = whole[0:1], whole[1:2]
    else:
        half = LANES // 2
        a = jnp.sum(total[2:3, :half], axis=1, keepdims=True)
        b = jnp.sum(total[2:3, half:], axis=1, keepdims=True)
    all_ref[...] = a / jnp.sqrt(b + 1.0)


def shards(nx, ny, weights, bin_ids):
    n = nx * ny
    vmem = pl.BlockSpec(memory_space=pltpu.VMEM)
    hbm = pl.BlockSpec(memory_space=pltpu.HBM)
    weights, bin_ids = weights.reshape(-1, LANES), bin_ids.reshape(-1, LANES)
    total = pl.pallas_call(
        functools.partial(kernel, nx, ny),
        out_shape=jax.ShapeDtypeStruct((ROWS, LANES), jnp.float32),
        in_specs=[hbm, hbm],
        out_specs=vmem,
        scratch_shapes=[
            pltpu.VMEM(weights.shape, weights.dtype),
            pltpu.VMEM(bin_ids.shape, bin_ids.dtype),
            pltpu.VMEM((n, ROWS, LANES), jnp.float32),
            pltpu.VMEM((n - 1, ROWS, LANES), jnp.float32),
            pltpu.SemaphoreType.DMA,
            pltpu.SemaphoreType.DMA,
            pltpu.SemaphoreType.DMA((2,)),
        ],
        compiler_params=pltpu.CompilerParams(
            collective_id=0, has_side_effects=True, vmem_limit_bytes=16 * 1024 * 1024
        ),
    )(*(pltpu.with_memory_space_constraint(a, pltpu.HBM) for a in (weights, bin_ids)))
    significance, overall = pl.pallas_call(
        finish_kernel,
        out_shape=(jax.ShapeDtypeStruct((1, LANES), jnp.float32), jax.ShapeDtypeStruct((1, 1), jnp.float32)),
        in_specs=[vmem],
        out_specs=(vmem, vmem),
        compiler_params=pltpu.CompilerParams(vmem_limit_bytes=16 * 1024 * 1024),
    )(total)
    return significance.reshape(LANES), overall.reshape(())


def solution(mesh):
    spec = P(("gx", "gy"))
    body = functools.partial(shards, mesh.shape["gx"], mesh.shape["gy"])
    return jax.shard_map(body, mesh=mesh, in_specs=(spec, spec), out_specs=(spec, P()), check_vma=False)
```
